32 devices in a mesh: gx: 8 (over z, core), gy: 4 (over y, x).
Axes of the slice: x: 2, y: 2, z: 4, core: 2. Of those that a mesh axis runs over, the one named last changes fastest.
Arguments:
- potential: float32 [32, 64, 256], P('gx', 'gy'), may hold values from -0.2 to 1.2
- recovery: float32 [32, 64, 256], P('gx', 'gy'), may hold values from 0 to 1.5
- fiber_angles: float32 [2, 32, 64, 256], P(None, 'gx', 'gy'), may hold values from -3.140625 to 3.140625
- deform: float32 [9, 8192], P(None, ('gx', 'gy')), may hold values from -0.15 to 1.25, as said below
- elem_slot: int32 [8, 16, 64], P('gx', 'gy'), may hold values from 0 to 8191, as said below
Outputs:
- potential_next: float32 [32, 64, 256], P('gx', 'gy')
- recovery_next: float32 [32, 64, 256], P('gx', 'gy')
The draws below stay inside these ranges and needn't reach their ends.
Inputs may be any that keep to these rules, and one draw needn't show every extreme that they name: `elem_slot`: entries are distinct. Slot s lies on device s / 256 (rounded down) of gx+gy. The elements of one device's block along gx and gy lie in the slots of the devices with the same index along gx, exactly 64 of them in each. `deform`: components 0, 4 and 8 (the diagonal of F) lie in 0.8 to 1.25, the other six in -0.15 to 0.15.
All inputs are finite; a program needn't handle non-finite values.
Results may differ from the reference program's by a relative error of at most 0.0003.
Values sent between devices are 32-bit elements; how exact they have to be, the bound alone decides.
A program may use at most 64 MiB of HBM per device.

```python
import math
import jax
import jax.numpy as jnp
from jax import lax

RATIO = 4
KX = 1
KY = 4
NCZ = 64
NZ = 256
NX = 32
NY = 64
CB = 256
SHARE = 64
NE = 8192
N_GX = 8
N_GY = 4
DEVICES = 32


def draw_deform(key, part):
    diag_key = jax.random.fold_in(key, 21)
    off_key = jax.random.fold_in(key, 22)
    diagonal = jnp.exp(jax.random.uniform(diag_key, (3, NE), jnp.float32, math.log(0.8), math.log(1.25)))
    offside = jnp.clip(0.06 * jax.random.normal(off_key, (6, NE), jnp.float32), -0.15, 0.15)
    diagonal = jnp.clip(diagonal, 0.8, 1.25)
    rows = [diagonal[0], offside[0], offside[1], offside[2], diagonal[1], offside[3], offside[4], offside[5], diagonal[2]]
    return jnp.stack(rows).astype(jnp.float32)


def draw_elem_slot(key, part):
    block_keys = jax.random.split(jax.random.fold_in(key, 31), DEVICES)
    holder_keys = jax.random.split(jax.random.fold_in(key, 32), DEVICES)
    ranks = jax.vmap(lambda one_key: jax.random.permutation(one_key, CB))(block_keys).astype(jnp.int32)
    holding = jax.vmap(lambda one_key: jax.random.permutation(one_key, CB))(holder_keys).astype(jnp.int32)
    device_index = jnp.arange(DEVICES, dtype=jnp.int32)
    row_start = device_index // N_GY * N_GY
    column = device_index % N_GY
    holder = row_start[:, None] + ranks // SHARE
    position = column[:, None] * SHARE + ranks % SHARE
    local_slot = holding[holder, position]
    slots = holder * CB + local_slot
    grid = slots.reshape(N_GX, N_GY, KX, KY, NCZ).transpose(0, 2, 1, 3, 4).reshape(N_GX * KX, N_GY * KY, NCZ)
    return grid.astype(jnp.int32)


def block_scale(key, dims, shards, smallest, largest):
    def one(dim, parts):
        draws = jax.random.uniform(jax.random.fold_in(jax.random.fold_in(key, 6), dim), (parts,), jnp.float32, smallest / len(shards), largest / len(shards))
        return jnp.repeat(jnp.exp(draws), dims[dim] // parts).reshape((-1,) + (1,) * (len(dims) - dim - 1))

    level = one(*shards[0])
    for cut in shards[1:]:
        level = level * one(*cut)
    return level


def setup_inputs(seed: int = 0) -> dict:
    seeds = jax.random.split(jax.random.key(seed), 6)
    potential = jnp.clip(-0.2 + 1.4000001 * jax.random.uniform(seeds[0], (NX, NY, NZ), jnp.float32) ** block_scale(seeds[0], (NX, NY, NZ), ((0, 8), (1, 4)), -0.2, 0.2), -0.2, 1.2)
    recovery = jnp.clip(1.5 * jax.random.uniform(seeds[1], (NX, NY, NZ), jnp.float32) ** block_scale(seeds[1], (NX, NY, NZ), ((0, 8), (1, 4)), -0.2, 0.2), 0.0, 1.5)
    fiber_angles = jnp.clip(jax.random.uniform(seeds[2], (2, NX, NY, NZ), jnp.float32, -3.140625, 3.140625), -3.140625, 3.140625)
    deform = draw_deform(jax.random.fold_in(seeds[5], 71), 0)
    elem_slot = draw_elem_slot(jax.random.fold_in(seeds[5], 71), 0)
    return dict(potential=potential, recovery=recovery, fiber_angles=fiber_angles, deform=deform, elem_slot=elem_slot)


sigma_fiber = 1.0
sigma_cross = 0.3
time_step = 0.1
excite_gain = 8.0
excite_level = 0.15
stretch_gain = 10.0
stretch_reversal = 0.6
recover_rate = 0.5

def refine(padded, dim):
    inner_size = padded.shape[dim] - 2
    lower = lax.slice_in_dim(padded, 0, inner_size, axis=dim)
    middle = lax.slice_in_dim(padded, 1, inner_size + 1, axis=dim)
    upper = lax.slice_in_dim(padded, 2, inner_size + 2, axis=dim)
    pieces = []
    for position in range(RATIO):
        offset = (position + 0.5) / RATIO - 0.5
        weight = abs(offset)
        neighbor = lower if offset < 0 else upper
        pieces.append((1.0 - weight) * middle + weight * neighbor)
    stacked = jnp.stack(pieces, axis=dim + 1)
    new_shape = list(padded.shape)
    new_shape[dim] = inner_size * RATIO
    return stacked.reshape(new_shape)

def directions(angles):
    azimuth = angles[0]
    elevation = angles[1]
    return jnp.stack([jnp.cos(azimuth) * jnp.cos(elevation), jnp.sin(azimuth) * jnp.cos(elevation), jnp.sin(elevation)])

def tensors(field, fiber):
    entries = [field[number] for number in range(9)]

    def element(row_index, col_index):
        return entries[3 * (row_index % 3) + col_index % 3]
    cofactor = [[element(row_index + 1, col_index + 1) * element(row_index + 2, col_index + 2) - element(row_index + 1, col_index + 2) * element(row_index + 2, col_index + 1) for col_index in range(3)] for row_index in range(3)]
    determinant = element(0, 0) * cofactor[0][0] + element(0, 1) * cofactor[0][1] + element(0, 2) * cofactor[0][2]
    inverse = [[cofactor[col_index][row_index] / determinant for col_index in range(3)] for row_index in range(3)]
    stretched = [element(row_index, 0) * fiber[0] + element(row_index, 1) * fiber[1] + element(row_index, 2) * fiber[2] for row_index in range(3)]
    stretch = jnp.sqrt(stretched[0] * stretched[0] + stretched[1] * stretched[1] + stretched[2] * stretched[2])
    pulled = [inverse[row_index][0] * fiber[0] + inverse[row_index][1] * fiber[1] + inverse[row_index][2] * fiber[2] for row_index in range(3)]
    conduct = []
    for first_index, second_index in ((0, 0), (1, 1), (2, 2), (0, 1), (0, 2), (1, 2)):
        metric = inverse[first_index][0] * inverse[second_index][0] + inverse[first_index][1] * inverse[second_index][1] + inverse[first_index][2] * inverse[second_index][2]
        conduct.append(sigma_cross * metric + (sigma_fiber - sigma_cross) * pulled[first_index] * pulled[second_index])
    return (jnp.stack(conduct), stretch)

def close_faces(flux, dim, at_first, at_last):
    extent = flux.shape[dim]
    face_index = lax.broadcasted_iota(jnp.int32, flux.shape, dim)
    closed = (face_index == 0) & at_first | (face_index == extent - 1) & at_last
    return jnp.where(closed, jnp.zeros_like(flux), flux)

def divergence(potential_pad, tensor_pad, first_x, last_x, first_y, last_y):
    grad_x = (potential_pad[2:, :, :] - potential_pad[:-2, :, :]) * 0.5
    grad_y = (potential_pad[:, 2:, :] - potential_pad[:, :-2, :]) * 0.5
    grad_z = (potential_pad[:, :, 2:] - potential_pad[:, :, :-2]) * 0.5

    def face_mean(component, dim):
        inner = tensor_pad[component]
        if dim == 0:
            inner = inner[:, 1:-1, 1:-1]
        elif dim == 1:
            inner = inner[1:-1, :, 1:-1]
        else:
            inner = inner[1:-1, 1:-1, :]
        extent = inner.shape[dim]
        return (lax.slice_in_dim(inner, 1, extent, axis=dim) + lax.slice_in_dim(inner, 0, extent - 1, axis=dim)) * 0.5
    step_x = potential_pad[1:, 1:-1, 1:-1] - potential_pad[:-1, 1:-1, 1:-1]
    mean_y = (grad_y[1:, :, 1:-1] + grad_y[:-1, :, 1:-1]) * 0.5
    mean_z = (grad_z[1:, 1:-1, :] + grad_z[:-1, 1:-1, :]) * 0.5
    flux_x = face_mean(0, 0) * step_x + face_mean(3, 0) * mean_y + face_mean(4, 0) * mean_z
    flux_x = close_faces(flux_x, 0, first_x, last_x)
    step_y = potential_pad[1:-1, 1:, 1:-1] - potential_pad[1:-1, :-1, 1:-1]
    mean_x = (grad_x[:, 1:, 1:-1] + grad_x[:, :-1, 1:-1]) * 0.5
    mean_z = (grad_z[1:-1, 1:, :] + grad_z[1:-1, :-1, :]) * 0.5
    flux_y = face_mean(3, 1) * mean_x + face_mean(1, 1) * step_y + face_mean(5, 1) * mean_z
    flux_y = close_faces(flux_y, 1, first_y, last_y)
    step_z = potential_pad[1:-1, 1:-1, 1:] - potential_pad[1:-1, 1:-1, :-1]
    mean_x = (grad_x[:, 1:-1, 1:] + grad_x[:, 1:-1, :-1]) * 0.5
    mean_y = (grad_y[1:-1, :, 1:] + grad_y[1:-1, :, :-1]) * 0.5
    flux_z = face_mean(4, 2) * mean_x + face_mean(5, 2) * mean_y + face_mean(2, 2) * step_z
    flux_z = close_faces(flux_z, 2, True, True)
    return flux_x[1:] - flux_x[:-1] + (flux_y[:, 1:] - flux_y[:, :-1]) + (flux_z[:, :, 1:] - flux_z[:, :, :-1])

def update(voltage, recovery, divergent, stretch):
    current = excite_gain * voltage * (voltage - excite_level) * (voltage - 1.0) + voltage * recovery
    current = current + stretch_gain * jnp.maximum(stretch - 1.0, 0.0) * (voltage - stretch_reversal)
    voltage_next = voltage + time_step * (divergent - current)
    recovery_next = recovery + time_step * recover_rate * (-recovery - excite_gain * voltage * (voltage - excite_level - 1.0))
    return (voltage_next, recovery_next)

def reference(potential, recovery, fiber_angles, deform, elem_slot):
    coarse = deform[:, elem_slot]
    coarse = jnp.pad(coarse, ((0, 0), (1, 1), (1, 1), (1, 1)), mode='edge')
    along_x = refine(coarse, 1)
    along_x = jnp.pad(along_x, ((0, 0), (1, 1), (0, 0), (0, 0)), mode='edge')
    angles_pad = jnp.pad(fiber_angles, ((0, 0), (1, 1), (0, 0), (0, 0)), mode='edge')
    potential_all = jnp.pad(potential, 1, mode='edge')
    width = NX // N_GX

    def slab(index):
        start = (index * width).astype(jnp.int32)
        segment = lax.dynamic_slice_in_dim(along_x, start, width + 2, axis=1)
        fine_field = refine(refine(segment, 2), 3)
        angles = lax.dynamic_slice_in_dim(angles_pad, start, width + 2, axis=1)
        conduct, stretch = tensors(fine_field, directions(angles))
        tensor_pad = jnp.pad(conduct, ((0, 0), (0, 0), (1, 1), (1, 1)), mode='edge')
        potential_pad = lax.dynamic_slice_in_dim(potential_all, start, width + 2, axis=0)
        divergent = divergence(potential_pad, tensor_pad, index == 0, index == N_GX - 1, True, True)
        voltage = lax.dynamic_slice_in_dim(potential, start, width, axis=0)
        resting = lax.dynamic_slice_in_dim(recovery, start, width, axis=0)
        return update(voltage, resting, divergent, stretch[1:-1])
    voltage_next, recovery_next = lax.map(slab, jnp.arange(N_GX, dtype=jnp.int32))
    return (voltage_next.reshape(NX, NY, NZ), recovery_next.reshape(NX, NY, NZ))
```

```python
import functools

import jax
import jax.numpy as jnp
from jax import lax
from jax.experimental import pallas as pl
from jax.experimental.pallas import tpu as pltpu
from jax.sharding import PartitionSpec as P

MESH = pl.DeviceIdType.MESH
RATIO = 4
LANES = 128
TOP = 8

SIDES = tuple((dx, dy) for dx in (-1, 0, 1) for dy in (-1, 0, 1) if (dx, dy) != (0, 0))


def split_two(values):
    high = values.astype(jnp.bfloat16)
    low = (values - high.astype(jnp.float32)).astype(jnp.bfloat16)
    return high, low


def dot_two(values, weights):
    high, low = split_two(values)
    return jnp.dot(high, weights, preferred_element_type=jnp.float32) + jnp.dot(
        low, weights, preferred_element_type=jnp.float32
    )


def sine_cosine(angle):
    turn = jnp.floor(angle * 0.6366197723675814 + 0.5)
    rest = angle - turn * 1.5703125
    rest = rest - turn * 4.8375129699707031e-4
    rest = rest - turn * 7.549789948768648e-8
    square = rest * rest
    sine = rest + rest * square * (
        -1.6666654611e-1 + square * (8.3321608736e-3 + square * -1.9515295891e-4)
    )
    cosine = (
        1.0
        - 0.5 * square
        + square
        * square
        * (4.166664568298827e-2 + square * (-1.388731625493765e-3 + square * 2.443315711809948e-5))
    )
    size = jnp.abs(turn)
    odd = size == 1.0
    sine_part = jnp.where(odd, cosine * turn, sine)
    cosine_part = jnp.where(odd, sine * -turn, cosine)
    flip = jnp.where(size == 2.0, -1.0, 1.0)
    return sine_part * flip, cosine_part * flip


def fiber_of(azimuth, elevation):
    sin_u, cos_u = sine_cosine(azimuth)
    sin_e, cos_e = sine_cosine(elevation)
    return cos_u * cos_e, sin_u * cos_e, sin_e


def tensor_of(entries, fiber):
    def element(i, j):
        return entries[3 * (i % 3) + j % 3]

    adjugate = [
        [
            element(j + 1, i + 1) * element(j + 2, i + 2)
            - element(j + 1, i + 2) * element(j + 2, i + 1)
            for j in range(3)
        ]
        for i in range(3)
    ]
    determinant = (
        element(0, 0) * adjugate[0][0]
        + element(0, 1) * adjugate[1][0]
        + element(0, 2) * adjugate[2][0]
    )
    inverse = 1.0 / determinant
    square = inverse * inverse
    cross = 0.3 * square
    along = 0.7 * square
    pulled = [
        adjugate[i][0] * fiber[0] + adjugate[i][1] * fiber[1] + adjugate[i][2] * fiber[2]
        for i in range(3)
    ]
    scaled = [along * pulled[i] for i in range(3)]
    conduct = []
    for i, j in ((0, 0), (1, 1), (2, 2), (0, 1), (0, 2), (1, 2)):
        metric = (
            adjugate[i][0] * adjugate[j][0]
            + adjugate[i][1] * adjugate[j][1]
            + adjugate[i][2] * adjugate[j][2]
        )
        conduct.append(cross * metric + scaled[i] * pulled[j])
    return conduct


def stretch_of(entries, fiber):
    parts = [
        entries[3 * i] * fiber[0] + entries[3 * i + 1] * fiber[1] + entries[3 * i + 2] * fiber[2]
        for i in range(3)
    ]
    return jnp.sqrt(parts[0] * parts[0] + parts[1] * parts[1] + parts[2] * parts[2])


def kernel(
    across,
    down,
    sizes,
    potential,
    recovery,
    angles,
    deform,
    slots,
    next_potential,
    next_recovery,
    volts,
    rest_in,
    own_angles,
    x_angles,
    y_angles,
    held,
    near_slots,
    fibers,
    conducts,
    stretches,
    send_sem,
    deform_sem,
    near_sem,
    local_sem,
):
    bx, by, nz, ex, ey, ez, parts, count = sizes
    gx, gy = lax.axis_index("gx"), lax.axis_index("gy")
    first_x, last_x = gx == 0, gx == across - 1
    first_y, last_y = gy == 0, gy == down - 1

    def exists(dx, dy):
        checks = []
        if dx:
            checks.append(jnp.logical_not(first_x if dx < 0 else last_x))
        if dy:
            checks.append(jnp.logical_not(first_y if dy < 0 else last_y))
        return checks[0] if len(checks) == 1 else jnp.logical_and(*checks)

    barrier = pltpu.get_barrier_semaphore()

    def row_targets(dx):
        for step in range(0 if dx else 1, down):
            yield step, lax.rem(gy + step, down)

    def greet(dx):
        for _, target in row_targets(dx):
            pl.semaphore_signal(barrier, inc=1, device_id=(gx + dx, target), device_id_type=MESH)

    pl.when(exists(-1, 0))(lambda: greet(-1))
    greet(0)
    pl.when(exists(1, 0))(lambda: greet(1))

    own = [
        pltpu.make_async_copy(
            potential, volts.at[pl.ds(1, bx), pl.ds(TOP, by), :], local_sem.at[0]
        ),
        pltpu.make_async_copy(recovery, rest_in, local_sem.at[1]),
        pltpu.make_async_copy(angles, own_angles, local_sem.at[2]),
        pltpu.make_async_copy(deform, held.at[1, gy], local_sem.at[3]),
        pltpu.make_async_copy(slots, near_slots.at[1, 1], local_sem.at[4]),
    ]
    for copy in (own[2], own[4], own[3], own[0], own[1]):
        copy.start()

    rows_here = 1 + jnp.where(first_x, 0, 1) + jnp.where(last_x, 0, 1)
    pl.semaphore_wait(barrier, rows_here * down - 1)

    def deform_copy(dx, step, target):
        index = (1 - dx) * down + step
        return pltpu.make_async_remote_copy(
            src_ref=deform,
            dst_ref=held.at[1 - dx, gy],
            send_sem=send_sem.at[index],
            recv_sem=deform_sem.at[index],
            device_id=(gx + dx, target),
            device_id_type=MESH,
        )

    def near_copies(dx, dy):
        place = (1 - dx) * 3 + (1 - dy)
        base = 3 * down + 3 * place
        x_source = pl.ds(0, bx) if dx == 0 else pl.ds(0 if dx < 0 else bx - 1, 1)
        x_target = pl.ds(1, bx) if dx == 0 else pl.ds(bx + 1 if dx < 0 else 0, 1)
        y_source = pl.ds(0, by) if dy == 0 else pl.ds(0 if dy < 0 else by - 1, 1)
        y_target = pl.ds(TOP, by) if dy == 0 else pl.ds(TOP + by if dy < 0 else TOP - 1, 1)
        pairs = [
            (slots, near_slots.at[1 - dx, 1 - dy]),
            (potential.at[x_source, y_source, :], volts.at[x_target, y_target, :]),
        ]
        if dy == 0:
            pairs.append((angles.at[:, x_source], x_angles.at[:, pl.ds(1 if dx < 0 else 0, 1)]))
        elif dx == 0:
            pairs.append((angles.at[:, :, y_source], y_angles.at[1 if dy < 0 else 0]))
        return [
            pltpu.make_async_remote_copy(
                src_ref=source,
                dst_ref=target,
                send_sem=send_sem.at[base + number],
                recv_sem=near_sem.at[3 * place + number],
                device_id=(gx + dx, gy + dy),
                device_id_type=MESH,
            )
            for number, (source, target) in enumerate(pairs)
        ]

    def over_row(dx, act):
        for step, target in row_targets(dx):
            act(deform_copy(dx, step, target))

    def over_near(dx, dy, act):
        for copy in near_copies(dx, dy):
            act(copy)

    def everything(act, way=1):
        def side(dx, dy):
            pl.when(exists(way * dx, way * dy))(lambda: over_near(dx, dy, act))

        for dx in (-1, 0, 1):
            if dx:
                pl.when(exists(way * dx, 0))(lambda dx=dx: over_row(dx, act))
            else:
                over_row(0, act)
        for dx, dy in SIDES:
            side(dx, dy)

    everything(lambda copy: copy.start())

    width = (ey + 2) * ez
    tall = by + 8
    row = lax.broadcasted_iota(jnp.int32, (tall, width), 0)
    lane = lax.broadcasted_iota(jnp.int32, (tall, width), 1)
    cell = jnp.where(row < by, row, jnp.where(row < by + bx, -1, by))
    spot = (cell.astype(jnp.float32) + 0.5) * (1.0 / RATIO) - 0.5
    weight_y = jnp.maximum(1.0 - jnp.abs(spot - ((lane // ez) - 1).astype(jnp.float32)), 0.0)
    row = lax.broadcasted_iota(jnp.int32, (width, nz), 0)
    lane = lax.broadcasted_iota(jnp.int32, (width, nz), 1)
    spot = jnp.clip((lane.astype(jnp.float32) + 0.5) * (1.0 / RATIO) - 0.5, 0.0, ez - 1.0)
    weight_z = jnp.maximum(1.0 - jnp.abs(spot - lax.rem(row, ez).astype(jnp.float32)), 0.0)
    weight_z = weight_z.astype(jnp.bfloat16)

    own[2].wait()
    for s in range(bx):
        for number, part in enumerate(fiber_of(own_angles[0, s], own_angles[1, s])):
            fibers[number, s + 1] = part

    for number in (4, 3, 0, 1):
        own[number].wait()

    everything(lambda copy: copy.wait_recv(), -1)

    gathered = []
    digits = lax.broadcasted_iota(jnp.int32, (LANES, width), 0)
    blocks = count // LANES
    for q in range(3):
        low = jnp.where(first_y, near_slots[q, 1, 0, 0:1], near_slots[q, 0, 0, ey - 1 : ey])
        high = jnp.where(last_y, near_slots[q, 1, 0, ey - 1 : ey], near_slots[q, 2, 0, 0:1])
        pieces = [low] + [near_slots[q, 1, 0, c : c + 1] for c in range(ey)] + [high]
        index = jnp.concatenate(pieces, axis=1) - (gx + q - 1) * (down * count)
        chosen = (digits == (index & (LANES - 1))).astype(jnp.float32).astype(jnp.bfloat16)
        table = []
        for h in range(down):
            block = held[q, h]
            block = jnp.concatenate([block, jnp.zeros((16 - parts, count), jnp.float32)], axis=0)
            table += [block[:, b * LANES : (b + 1) * LANES] for b in range(blocks)]
        found = dot_two(jnp.concatenate(table, axis=0), chosen)
        page = index >> (LANES.bit_length() - 1)
        total = jnp.zeros((16, width), jnp.float32)
        for h in range(down * blocks):
            total = jnp.where(page == h, found[16 * h : 16 * h + 16], total)
        gathered.append(total)
    gathered[0] = jnp.where(first_x, gathered[1], gathered[0])
    gathered[2] = jnp.where(last_x, gathered[1], gathered[2])

    refined = []
    for q in range(3):
        spread = [weight_y * gathered[q][k : k + 1] for k in range(parts)]
        refined.append(dot_two(jnp.concatenate(spread, axis=0), weight_z))

    @pl.when(first_y)
    def _():
        volts[:, TOP - 1 : TOP] = volts[:, TOP : TOP + 1]

    @pl.when(last_y)
    def _():
        volts[:, TOP + by : TOP + by + 1] = volts[:, TOP + by - 1 : TOP + by]

    @pl.when(first_x)
    def _():
        volts[0] = volts[1]

    @pl.when(last_x)
    def _():
        volts[bx + 1] = volts[bx]

    for side, s in ((0, 0), (1, bx + 1)):
        for number, part in enumerate(fiber_of(x_angles[0, side], x_angles[1, side])):
            fibers[number, s] = part
    rim = [
        jnp.concatenate([y_angles[side, c, s] for side in range(2) for s in range(bx)], axis=0)
        for c in range(2)
    ]
    rim_fiber = fiber_of(rim[0], rim[1])

    def hat(s):
        spot = (s + 0.5) / RATIO - 0.5
        return [max(0.0, 1.0 - abs(spot - (q - 1))) for q in range(3)]

    for s in range(bx + 2):
        weights = hat(s - 1)
        for half in range(by // 8):
            rows = slice(8 * half, 8 * half + 8)
            entries = []
            for k in range(parts):
                at = tall * k + 8 * half
                terms = [w * refined[q][at : at + 8] for q, w in enumerate(weights) if w]
                entries.append(functools.reduce(jnp.add, terms))
            fiber = [fibers[number, s, rows] for number in range(3)]
            for number, value in enumerate(tensor_of(entries, fiber)):
                conducts[number, s, TOP + 8 * half : TOP + 8 * half + 8] = value
            if 1 <= s <= bx:
                stretches[s - 1, rows] = stretch_of(entries, fiber)
    rim_row = lax.rem(lax.broadcasted_iota(jnp.int32, (2 * bx, nz), 0), bx).astype(jnp.float32)
    spot = (rim_row + 0.5) * (1.0 / RATIO) - 0.5
    rim_weights = [jnp.maximum(1.0 - jnp.abs(spot - (q - 1.0)), 0.0) for q in range(3)]
    entries = []
    for k in range(parts):
        at = tall * k + by
        entries.append(
            functools.reduce(
                jnp.add, [rim_weights[q] * refined[q][at : at + 2 * bx] for q in range(3)]
            )
        )
    for number, value in enumerate(tensor_of(entries, rim_fiber)):
        for s in range(bx):
            conducts[number, s + 1, TOP - 1 : TOP] = value[s : s + 1]
            conducts[number, s + 1, TOP + by : TOP + by + 1] = value[bx + s : bx + s + 1]

    z_lane = lax.broadcasted_iota(jnp.int32, (by, nz), 1)
    y_row = lax.broadcasted_iota(jnp.int32, (by, nz), 0)

    def next_z(values):
        return jnp.where(z_lane == nz - 1, values, pltpu.roll(values, nz - 1, 1))

    def last_z(values):
        return jnp.where(z_lane == 0, values, pltpu.roll(values, 1, 1))

    def grad_z(values):
        return next_z(values) - last_z(values)

    def at(s, shift):
        return volts[s, TOP + shift : TOP + shift + by]

    def tensor(number, s, shift=0):
        return conducts[number, s, TOP + shift : TOP + shift + by]

    XX, YY, ZZ, XY, XZ, YZ = range(6)
    middle = [at(s, 0) for s in range(bx + 2)]
    grads_y = [at(s, 1) - at(s, -1) for s in range(bx + 2)]
    grads_z = [grad_z(middle[s]) for s in range(bx + 2)]

    def face_x(f):
        def mean(number):
            return tensor(number, f) + tensor(number, f + 1)

        return (
            0.5 * mean(XX) * (middle[f + 1] - middle[f])
            + 0.125 * mean(XY) * (grads_y[f] + grads_y[f + 1])
            + 0.125 * mean(XZ) * (grads_z[f] + grads_z[f + 1])
        )

    faces = [face_x(f) for f in range(bx + 1)]
    faces[0] = jnp.where(first_x, 0.0, faces[0])
    faces[bx] = jnp.where(last_x, 0.0, faces[bx])

    for i in range(bx):
        s = i + 1
        grad_x = middle[s + 1] - middle[s - 1]

        def face_y(shift):
            def mean(number):
                return tensor(number, s) + tensor(number, s, shift)

            step = (at(s, shift) - middle[s]) * (1.0 if shift > 0 else -1.0)
            other_x = at(s + 1, shift) - at(s - 1, shift)
            return (
                0.125 * mean(XY) * (grad_x + other_x)
                + 0.5 * mean(YY) * step
                + 0.125 * mean(YZ) * (grads_z[s] + grad_z(at(s, shift)))
            )

        upper = jnp.where(jnp.logical_and(y_row == by - 1, last_y), 0.0, face_y(1))
        lower = jnp.where(jnp.logical_and(y_row == 0, first_y), 0.0, face_y(-1))

        def pair(values):
            return values + next_z(values)

        face_z = (
            0.125 * pair(tensor(XZ, s)) * pair(grad_x)
            + 0.125 * pair(tensor(YZ, s)) * pair(grads_y[s])
            + 0.5 * pair(tensor(ZZ, s)) * (next_z(middle[s]) - middle[s])
        )
        face_z = jnp.where(z_lane == nz - 1, 0.0, face_z)
        divergent = (
            (faces[i + 1] - faces[i]) + (upper - lower) + (face_z - pltpu.roll(face_z, 1, 1))
        )
        voltage = middle[s]
        resting = rest_in[i]
        current = 8.0 * voltage * (voltage - 0.15) * (voltage - 1.0) + voltage * resting
        current = current + 10.0 * jnp.maximum(stretches[i] - 1.0, 0.0) * (voltage - 0.6)
        next_potential[i] = voltage + 0.1 * (divergent - current)
        next_recovery[i] = resting + 0.05 * (-resting - 8.0 * voltage * (voltage - 1.15))

    everything(lambda copy: copy.wait_send())


def solution(mesh):
    across, down = mesh.shape["gx"], mesh.shape["gy"]

    def local(potential, recovery, angles, deform, slots):
        bx, by, nz = potential.shape
        ex, ey, ez = slots.shape
        parts, count = deform.shape
        assert ex == 1 and bx == RATIO and by % 8 == 0 and count % LANES == 0
        sizes = (bx, by, nz, ex, ey, ez, parts, count)
        f32 = jnp.float32
        shape = jax.ShapeDtypeStruct(potential.shape, f32)
        copies = 3 * down + 27
        return pl.pallas_call(
            functools.partial(kernel, across, down, sizes),
            out_shape=(shape, shape),
            in_specs=[pl.BlockSpec(memory_space=pl.ANY)] * 5,
            out_specs=(pl.BlockSpec(memory_space=pltpu.VMEM),) * 2,
            scratch_shapes=[
                pltpu.VMEM((bx + 2, by + 16, nz), f32),
                pltpu.VMEM(recovery.shape, f32),
                pltpu.VMEM(angles.shape, f32),
                pltpu.VMEM((2, 2, by, nz), f32),
                pltpu.VMEM((2, 2, bx, 1, nz), f32),
                pltpu.VMEM((3, down, parts, count), f32),
                pltpu.VMEM((3, 3, ex, ey, ez), jnp.int32),
                pltpu.VMEM((3, bx + 2, by, nz), f32),
                pltpu.VMEM((6, bx + 2, by + 16, nz), f32),
                pltpu.VMEM((bx, by, nz), f32),
                pltpu.SemaphoreType.DMA((copies,)),
                pltpu.SemaphoreType.DMA((3 * down,)),
                pltpu.SemaphoreType.DMA((27,)),
                pltpu.SemaphoreType.DMA((5,)),
            ],
            compiler_params=pltpu.CompilerParams(collective_id=0, has_side_effects=True),
        )(potential, recovery, angles, deform, slots)

    return jax.shard_map(
        local,
        mesh=mesh,
        in_specs=(
            P("gx", "gy", None),
            P("gx", "gy", None),
            P(None, "gx", "gy", None),
            P(None, ("gx", "gy")),
            P("gx", "gy", None),
        ),
        out_specs=(P("gx", "gy", None), P("gx", "gy", None)),
        check_vma=False,
    )
```

```python
import functools

import jax
import jax.numpy as jnp
from jax import lax
from jax.experimental import pallas as pl
from jax.experimental.pallas import tpu as pltpu
from jax.sharding import PartitionSpec as P

MESH = pl.DeviceIdType.MESH
RATIO = 4
LANES = 128
VMEM_LIMIT = 16 * 1024 * 1024
TOP = 8

SIDES = tuple((dx, dy) for dx in (-1, 0, 1) for dy in (-1, 0, 1) if (dx, dy) != (0, 0))


def split_two(values):
    high = values.astype(jnp.bfloat16)
    low = (values - high.astype(jnp.float32)).astype(jnp.bfloat16)
    return high, low


def dot_two(values, weights):
    high, low = split_two(values)
    return jnp.dot(high, weights, preferred_element_type=jnp.float32) + jnp.dot(
        low, weights, preferred_element_type=jnp.float32
    )


def sine_cosine(angle):
    turn = jnp.floor(angle * 0.6366197723675814 + 0.5)
    rest = angle - turn * 1.5703125
    rest = rest - turn * 4.8375129699707031e-4
    rest = rest - turn * 7.549789948768648e-8
    square = rest * rest
    sine = rest + rest * square * (
        -1.6666654611e-1 + square * (8.3321608736e-3 + square * -1.9515295891e-4)
    )
    cosine = (
        1.0
        - 0.5 * square
        + square
        * square
        * (4.166664568298827e-2 + square * (-1.388731625493765e-3 + square * 2.443315711809948e-5))
    )
    size = jnp.abs(turn)
    odd = size == 1.0
    sine_part = jnp.where(odd, cosine * turn, sine)
    cosine_part = jnp.where(odd, sine * -turn, cosine)
    flip = jnp.where(size == 2.0, -1.0, 1.0)
    return sine_part * flip, cosine_part * flip


def fiber_of(azimuth, elevation):
    sin_u, cos_u = sine_cosine(azimuth)
    sin_e, cos_e = sine_cosine(elevation)
    return cos_u * cos_e, sin_u * cos_e, sin_e


def tensor_of(entries, fiber):
    def element(i, j):
        return entries[3 * (i % 3) + j % 3]

    adjugate = [
        [
            element(j + 1, i + 1) * element(j + 2, i + 2)
            - element(j + 1, i + 2) * element(j + 2, i + 1)
            for j in range(3)
        ]
        for i in range(3)
    ]
    determinant = (
        element(0, 0) * adjugate[0][0]
        + element(0, 1) * adjugate[1][0]
        + element(0, 2) * adjugate[2][0]
    )
    inverse = 1.0 / determinant
    square = inverse * inverse
    cross = 0.3 * square
    along = 0.7 * square
    pulled = [
        adjugate[i][0] * fiber[0] + adjugate[i][1] * fiber[1] + adjugate[i][2] * fiber[2]
        for i in range(3)
    ]
    scaled = [along * pulled[i] for i in range(3)]
    conduct = []
    for i, j in ((0, 0), (1, 1), (2, 2), (0, 1), (0, 2), (1, 2)):
        metric = (
            adjugate[i][0] * adjugate[j][0]
            + adjugate[i][1] * adjugate[j][1]
            + adjugate[i][2] * adjugate[j][2]
        )
        conduct.append(cross * metric + scaled[i] * pulled[j])
    return conduct


def stretch_of(entries, fiber):
    parts = [
        entries[3 * i] * fiber[0] + entries[3 * i + 1] * fiber[1] + entries[3 * i + 2] * fiber[2]
        for i in range(3)
    ]
    return jnp.sqrt(parts[0] * parts[0] + parts[1] * parts[1] + parts[2] * parts[2])


def exchange(
    across,
    down,
    sizes,
    potential,
    recovery,
    angles,
    deform,
    slots,
    cells,
    rest_in,
    held,
    near_slots,
    fibers,
    spread_y,
    spread_z,
    send_sem,
    deform_sem,
    near_sem,
    local_sem,
):
    bx, by, nz, ex, ey, ez, parts, count = sizes
    blocks = count // LANES
    gx, gy = lax.axis_index("gx"), lax.axis_index("gy")
    first_x, last_x = gx == 0, gx == across - 1
    first_y, last_y = gy == 0, gy == down - 1

    def exists(dx, dy):
        checks = []
        if dx:
            checks.append(jnp.logical_not(first_x if dx < 0 else last_x))
        if dy:
            checks.append(jnp.logical_not(first_y if dy < 0 else last_y))
        return checks[0] if len(checks) == 1 else jnp.logical_and(*checks)

    barrier = pltpu.get_barrier_semaphore()

    def row_targets(dx):
        for step in range(0 if dx else 1, down):
            yield step, lax.rem(gy + step, down)

    def greet(dx):
        for _, target in row_targets(dx):
            pl.semaphore_signal(barrier, inc=1, device_id=(gx + dx, target), device_id_type=MESH)

    pl.when(exists(-1, 0))(lambda: greet(-1))
    pl.when(exists(1, 0))(lambda: greet(1))
    greet(0)

    packed = held.at[1, gy]
    local = []

    def fetch(source, target):
        copy = pltpu.make_async_copy(source, target, local_sem.at[len(local)])
        copy.start()
        local.append(copy)

    for b in range(blocks):
        columns = pl.ds(b * LANES, LANES)
        fetch(deform.at[pl.ds(0, 8), columns], packed.at[pl.ds(8 * b, 8)])
        fetch(deform.at[pl.ds(8, 1), columns], packed.at[pl.ds(8 * blocks + b, 1)])
    fetch(slots, near_slots.at[1, 1])
    inside = pl.ds(TOP, by)
    fetch(potential, cells.at[0, pl.ds(1, bx), inside])
    fetch(angles, cells.at[pl.ds(1, 2), pl.ds(1, bx), inside])
    fetch(recovery, rest_in)
    for copy in local:
        copy.wait()

    rows_here = 1 + jnp.where(first_x, 0, 1) + jnp.where(last_x, 0, 1)
    pl.semaphore_wait(barrier, rows_here * down - 1)

    def deform_copy(dx, step, target):
        index = (1 - dx) * down + step
        rows = pl.ds(0, 9 * blocks)
        return pltpu.make_async_remote_copy(
            src_ref=held.at[1, gy, rows],
            dst_ref=held.at[1 - dx, gy, rows],
            send_sem=send_sem.at[index],
            recv_sem=deform_sem.at[index],
            device_id=(gx + dx, target),
            device_id_type=MESH,
        )

    def near_copies(dx, dy):
        place = (1 - dx) * 3 + (1 - dy)
        base = 3 * down + 2 * place
        x_source = pl.ds(1, bx) if dx == 0 else pl.ds(1 if dx < 0 else bx, 1)
        x_target = pl.ds(1, bx) if dx == 0 else pl.ds(bx + 1 if dx < 0 else 0, 1)
        y_source = inside if dy == 0 else pl.ds(TOP if dy < 0 else TOP + by - 1, 1)
        y_target = inside if dy == 0 else pl.ds(TOP + by if dy < 0 else TOP - 1, 1)
        fields = pl.ds(0, 1 if dx and dy else 3)
        pairs = [
            (near_slots.at[1, 1], near_slots.at[1 - dx, 1 - dy]),
            (cells.at[fields, x_source, y_source], cells.at[fields, x_target, y_target]),
        ]
        return [
            pltpu.make_async_remote_copy(
                src_ref=source,
                dst_ref=target,
                send_sem=send_sem.at[base + number],
                recv_sem=near_sem.at[2 * place + number],
                device_id=(gx + dx, gy + dy),
                device_id_type=MESH,
            )
            for number, (source, target) in enumerate(pairs)
        ]

    def over_row(dx, act):
        for step, target in row_targets(dx):
            act(deform_copy(dx, step, target))

    def over_near(dx, dy, act):
        for copy in near_copies(dx, dy):
            act(copy)

    def everything(act, way=1):
        def side(dx, dy):
            pl.when(exists(way * dx, way * dy))(lambda: over_near(dx, dy, act))

        for dx in (-1, 1, 0):
            if dx:
                pl.when(exists(way * dx, 0))(lambda dx=dx: over_row(dx, act))
            else:
                over_row(0, act)
        for dx, dy in SIDES:
            side(dx, dy)

    everything(lambda copy: copy.start())

    width = (ey + 2) * ez
    tall = by + 8
    row = lax.broadcasted_iota(jnp.int32, (tall, width), 0)
    lane = lax.broadcasted_iota(jnp.int32, (tall, width), 1)
    cell = jnp.where(row < by, row, jnp.where(row < by + bx, -1, by))
    spot = (cell.astype(jnp.float32) + 0.5) * (1.0 / RATIO) - 0.5
    spread_y[...] = jnp.maximum(
        1.0 - jnp.abs(spot - ((lane // ez) - 1).astype(jnp.float32)), 0.0
    )
    row = lax.broadcasted_iota(jnp.int32, (width, nz), 0)
    lane = lax.broadcasted_iota(jnp.int32, (width, nz), 1)
    spot = jnp.clip((lane.astype(jnp.float32) + 0.5) * (1.0 / RATIO) - 0.5, 0.0, ez - 1.0)
    weight = jnp.maximum(1.0 - jnp.abs(spot - lax.rem(row, ez).astype(jnp.float32)), 0.0)
    spread_z[...] = weight.astype(jnp.bfloat16)

    for s in range(bx):
        own = [cells[number, s + 1, TOP : TOP + by] for number in (1, 2)]
        for number, part in enumerate(fiber_of(*own)):
            fibers[number, s] = part

    everything(lambda copy: copy.wait_recv(), -1)
    everything(lambda copy: copy.wait_send())


def compute(
    across,
    down,
    sizes,
    cells,
    rest_in,
    held,
    near_slots,
    fibers,
    spread_y,
    spread_z,
    next_potential,
    next_recovery,
    volts,
    conducts,
    out_potential,
    out_recovery,
    out_sem,
):
    bx, by, nz, ex, ey, ez, parts, count = sizes
    blocks = count // LANES
    gx, gy = lax.axis_index("gx"), lax.axis_index("gy")
    first_x, last_x = gx == 0, gx == across - 1
    first_y, last_y = gy == 0, gy == down - 1
    width = (ey + 2) * ez
    tall = by + 8

    for i in range(bx):
        voltage = cells[0, i + 1, TOP : TOP + by]
        resting = rest_in[i]
        out_recovery[i] = resting + 0.05 * (-resting - 8.0 * voltage * (voltage - 1.15))
    leaving = [pltpu.make_async_copy(out_recovery, next_recovery, out_sem.at[bx])]
    leaving[0].start()

    gathered = []
    digits = lax.broadcasted_iota(jnp.int32, (LANES, width), 0)
    pages = down * blocks
    for q in range(3):
        low = jnp.where(first_y, near_slots[q, 1, 0, 0:1], near_slots[q, 0, 0, ey - 1 : ey])
        high = jnp.where(last_y, near_slots[q, 1, 0, ey - 1 : ey], near_slots[q, 2, 0, 0:1])
        pieces = [low] + [near_slots[q, 1, 0, c : c + 1] for c in range(ey)] + [high]
        index = jnp.concatenate(pieces, axis=1) - (gx + q - 1) * (down * count)
        chosen = (digits == (index & (LANES - 1))).astype(jnp.float32).astype(jnp.bfloat16)
        table = [held[q, h, 0 : 8 * blocks] for h in range(down)]
        table += [held[q, h, 8 * blocks : 9 * blocks] for h in range(down)]
        found = dot_two(jnp.concatenate(table, axis=0), chosen)
        page = index >> (LANES.bit_length() - 1)
        total = jnp.zeros((8, width), jnp.float32)
        for h in range(pages):
            total = jnp.where(page == h, found[8 * h : 8 * h + 8], total)
        last = found[8 * pages : 9 * pages]
        kept = lax.broadcasted_iota(jnp.int32, (pages, width), 0) == page
        last = jnp.sum(jnp.where(kept, last, 0.0), axis=0, keepdims=True)
        gathered.append([total, last])
    for part in range(2):
        gathered[0][part] = jnp.where(first_x, gathered[1][part], gathered[0][part])
        gathered[2][part] = jnp.where(last_x, gathered[1][part], gathered[2][part])

    refined = []
    weight_y = spread_y[...]
    weight_z = spread_z[...]
    for q in range(3):
        total, last = gathered[q]
        spread = [weight_y * total[k : k + 1] for k in range(8)] + [weight_y * last]
        refined.append(dot_two(jnp.concatenate(spread, axis=0), weight_z))

    volts[...] = cells[0, :, 0:by + 16]

    @pl.when(first_y)
    def _():
        volts[:, TOP - 1 : TOP] = volts[:, TOP : TOP + 1]

    @pl.when(last_y)
    def _():
        volts[:, TOP + by : TOP + by + 1] = volts[:, TOP + by - 1 : TOP + by]

    @pl.when(first_x)
    def _():
        volts[0] = volts[1]

    @pl.when(last_x)
    def _():
        volts[bx + 1] = volts[bx]

    def rim_of(number):
        rows = [cells[number, s + 1, row : row + 1] for row in (TOP - 1, TOP + by) for s in range(bx)]
        return jnp.concatenate(rows, axis=0)

    rim = [rim_of(1), rim_of(2)]
    rim_fiber = fiber_of(rim[0], rim[1])

    def hat(s):
        spot = (s + 0.5) / RATIO - 0.5
        return [max(0.0, 1.0 - abs(spot - (q - 1))) for q in range(3)]

    for s in range(bx + 2):
        weights = hat(s - 1)
        for half in range(by // 8):
            rows = slice(8 * half, 8 * half + 8)
            entries = []
            for k in range(parts):
                at = tall * k + 8 * half
                terms = [w * refined[q][at : at + 8] for q, w in enumerate(weights) if w]
                entries.append(functools.reduce(jnp.add, terms))
            if 1 <= s <= bx:
                fiber = [fibers[number, s - 1, rows] for number in range(3)]
            else:
                fiber = fiber_of(*(cells[number, s, TOP + 8 * half : TOP + 8 * half + 8] for number in (1, 2)))
            for number, value in enumerate(tensor_of(entries, fiber)):
                conducts[number, s, TOP + 8 * half : TOP + 8 * half + 8] = value
            if 1 <= s <= bx:
                out_potential[s - 1, rows] = stretch_of(entries, fiber)
    rim_row = lax.rem(lax.broadcasted_iota(jnp.int32, (2 * bx, nz), 0), bx).astype(jnp.float32)
    spot = (rim_row + 0.5) * (1.0 / RATIO) - 0.5
    rim_weights = [jnp.maximum(1.0 - jnp.abs(spot - (q - 1.0)), 0.0) for q in range(3)]
    entries = []
    for k in range(parts):
        at = tall * k + by
        entries.append(
            functools.reduce(
                jnp.add, [rim_weights[q] * refined[q][at : at + 2 * bx] for q in range(3)]
            )
        )
    for number, value in enumerate(tensor_of(entries, rim_fiber)):
        for s in range(bx):
            conducts[number, s + 1, TOP - 1 : TOP] = value[s : s + 1]
            conducts[number, s + 1, TOP + by : TOP + by + 1] = value[bx + s : bx + s + 1]

    z_lane = lax.broadcasted_iota(jnp.int32, (by, nz), 1)
    y_row = lax.broadcasted_iota(jnp.int32, (by, nz), 0)

    def next_z(values):
        return jnp.where(z_lane == nz - 1, values, pltpu.roll(values, nz - 1, 1))

    def last_z(values):
        return jnp.where(z_lane == 0, values, pltpu.roll(values, 1, 1))

    def grad_z(values):
        return next_z(values) - last_z(values)

    def at(s, shift):
        return volts[s, TOP + shift : TOP + shift + by]

    def tensor(number, s, shift=0):
        return conducts[number, s, TOP + shift : TOP + shift + by]

    XX, YY, ZZ, XY, XZ, YZ = range(6)
    middle = [at(s, 0) for s in range(bx + 2)]
    grads_y = [at(s, 1) - at(s, -1) for s in range(bx + 2)]
    grads_z = [grad_z(middle[s]) for s in range(bx + 2)]

    def face_x(f):
        def mean(number):
            return tensor(number, f) + tensor(number, f + 1)

        return (
            0.5 * mean(XX) * (middle[f + 1] - middle[f])
            + 0.125 * mean(XY) * (grads_y[f] + grads_y[f + 1])
            + 0.125 * mean(XZ) * (grads_z[f] + grads_z[f + 1])
        )

    faces = [face_x(f) for f in range(bx + 1)]
    faces[0] = jnp.where(first_x, 0.0, faces[0])
    faces[bx] = jnp.where(last_x, 0.0, faces[bx])

    for i in range(bx):
        s = i + 1
        grad_x = middle[s + 1] - middle[s - 1]

        def face_y(shift):
            def mean(number):
                return tensor(number, s) + tensor(number, s, shift)

            step = (at(s, shift) - middle[s]) * (1.0 if shift > 0 else -1.0)
            other_x = at(s + 1, shift) - at(s - 1, shift)
            return (
                0.125 * mean(XY) * (grad_x + other_x)
                + 0.5 * mean(YY) * step
                + 0.125 * mean(YZ) * (grads_z[s] + grad_z(at(s, shift)))
            )

        upper = jnp.where(jnp.logical_and(y_row == by - 1, last_y), 0.0, face_y(1))
        lower = jnp.where(jnp.logical_and(y_row == 0, first_y), 0.0, face_y(-1))

        def pair(values):
            return values + next_z(values)

        face_z = (
            0.125 * pair(tensor(XZ, s)) * pair(grad_x)
            + 0.125 * pair(tensor(YZ, s)) * pair(grads_y[s])
            + 0.5 * pair(tensor(ZZ, s)) * (next_z(middle[s]) - middle[s])
        )
        face_z = jnp.where(z_lane == nz - 1, 0.0, face_z)
        divergent = (
            (faces[i + 1] - faces[i]) + (upper - lower) + (face_z - pltpu.roll(face_z, 1, 1))
        )
        voltage = middle[s]
        resting = rest_in[i]
        current = 8.0 * voltage * (voltage - 0.15) * (voltage - 1.0) + voltage * resting
        current = current + 10.0 * jnp.maximum(out_potential[i] - 1.0, 0.0) * (voltage - 0.6)
        out_potential[i] = voltage + 0.1 * (divergent - current)
        copy = pltpu.make_async_copy(out_potential.at[i], next_potential.at[i], out_sem.at[i])
        copy.start()
        leaving.append(copy)
    for copy in leaving:
        copy.wait()


def solution(mesh):
    across, down = mesh.shape["gx"], mesh.shape["gy"]

    def local(potential, recovery, angles, deform, slots):
        bx, by, nz = potential.shape
        ex, ey, ez = slots.shape
        parts, count = deform.shape
        assert ex == 1 and bx == RATIO and by % 8 == 0 and count % LANES == 0 and parts == 9
        sizes = (bx, by, nz, ex, ey, ez, parts, count)
        blocks = count // LANES
        width = (ey + 2) * ez
        f32 = jnp.float32
        shape = jax.ShapeDtypeStruct(potential.shape, f32)
        anywhere = pl.BlockSpec(memory_space=pl.ANY)
        in_vmem = pl.BlockSpec(memory_space=pltpu.VMEM)
        passed = (
            pltpu.VMEM((3, bx + 2, by + 16, nz), f32),
            pltpu.VMEM(recovery.shape, f32),
            pltpu.VMEM((3, down, 8 * blocks + 8, LANES), f32),
            pltpu.VMEM((3, 3, ex, ey, ez), jnp.int32),
            pltpu.VMEM((3, bx, by, nz), f32),
            pltpu.VMEM((by + 8, width), f32),
            pltpu.VMEM((width, nz), jnp.bfloat16),
        )
        arrived = pl.pallas_call(
            functools.partial(exchange, across, down, sizes),
            out_shape=passed,
            in_specs=[pl.BlockSpec(memory_space=pltpu.MemorySpace.HBM)] * 5,
            out_specs=(in_vmem,) * len(passed),
            scratch_shapes=[
                pltpu.SemaphoreType.DMA((3 * down + 18,)),
                pltpu.SemaphoreType.DMA((3 * down,)),
                pltpu.SemaphoreType.DMA((18,)),
                pltpu.SemaphoreType.DMA((2 * blocks + 4,)),
            ],
            compiler_params=pltpu.CompilerParams(
                collective_id=0, has_side_effects=True, vmem_limit_bytes=VMEM_LIMIT
            ),
        )(*(pltpu.with_memory_space_constraint(x, pltpu.MemorySpace.HBM) for x in (potential, recovery, angles, deform, slots)))
        return pl.pallas_call(
            functools.partial(compute, across, down, sizes),
            out_shape=(shape, shape),
            in_specs=[in_vmem] * len(passed),
            out_specs=(anywhere,) * 2,
            scratch_shapes=[
                pltpu.VMEM((bx + 2, by + 16, nz), f32),
                pltpu.VMEM((6, bx + 2, by + 16, nz), f32),
                pltpu.VMEM((bx, by, nz), f32),
                pltpu.VMEM((bx, by, nz), f32),
                pltpu.SemaphoreType.DMA((bx + 1,)),
            ],
            compiler_params=pltpu.CompilerParams(vmem_limit_bytes=VMEM_LIMIT),
        )(*arrived)

    return jax.shard_map(
        local,
        mesh=mesh,
        in_specs=(
            P("gx", "gy", None),
            P("gx", "gy", None),
            P(None, "gx", "gy", None),
            P(None, ("gx", "gy")),
            P("gx", "gy", None),
        ),
        out_specs=(P("gx", "gy", None), P("gx", "gy", None)),
        check_vma=False,
    )
```

```python
import functools

import jax
import jax.numpy as jnp
from jax import lax
from jax.experimental import pallas as pl
from jax.experimental.pallas import tpu as pltpu
from jax.sharding import PartitionSpec as P

MESH = pl.DeviceIdType.MESH
RATIO = 4
LANES = 128
VMEM_LIMIT = 16 * 1024 * 1024
TOP = 8

SIDES = tuple((dx, dy) for dx in (-1, 0, 1) for dy in (-1, 0, 1) if (dx, dy) != (0, 0))


def split_two(values):
    high = values.astype(jnp.bfloat16)
    low = (values - high.astype(jnp.float32)).astype(jnp.bfloat16)
    return high, low


def dot_two(values, weights):
    high, low = split_two(values)
    return jnp.dot(high, weights, preferred_element_type=jnp.float32) + jnp.dot(
        low, weights, preferred_element_type=jnp.float32
    )


def sine_cosine(angle):
    turn = jnp.floor(angle * 0.6366197723675814 + 0.5)
    rest = angle - turn * 1.5703125
    rest = rest - turn * 4.8375129699707031e-4
    rest = rest - turn * 7.549789948768648e-8
    square = rest * rest
    sine = rest + rest * square * (
        -1.6666654611e-1 + square * (8.3321608736e-3 + square * -1.9515295891e-4)
    )
    cosine = (
        1.0
        - 0.5 * square
        + square
        * square
        * (4.166664568298827e-2 + square * (-1.388731625493765e-3 + square * 2.443315711809948e-5))
    )
    size = jnp.abs(turn)
    odd = size == 1.0
    sine_part = jnp.where(odd, cosine * turn, sine)
    cosine_part = jnp.where(odd, sine * -turn, cosine)
    flip = jnp.where(size == 2.0, -1.0, 1.0)
    return sine_part * flip, cosine_part * flip


def fiber_of(azimuth, elevation):
    sin_u, cos_u = sine_cosine(azimuth)
    sin_e, cos_e = sine_cosine(elevation)
    return cos_u * cos_e, sin_u * cos_e, sin_e


def tensor_of(entries, fiber):
    def element(i, j):
        return entries[3 * (i % 3) + j % 3]

    adjugate = [
        [
            element(j + 1, i + 1) * element(j + 2, i + 2)
            - element(j + 1, i + 2) * element(j + 2, i + 1)
            for j in range(3)
        ]
        for i in range(3)
    ]
    determinant = (
        element(0, 0) * adjugate[0][0]
        + element(0, 1) * adjugate[1][0]
        + element(0, 2) * adjugate[2][0]
    )
    inverse = 1.0 / determinant
    square = inverse * inverse
    cross = 0.3 * square
    along = 0.7 * square
    pulled = [
        adjugate[i][0] * fiber[0] + adjugate[i][1] * fiber[1] + adjugate[i][2] * fiber[2]
        for i in range(3)
    ]
    scaled = [along * pulled[i] for i in range(3)]
    conduct = []
    for i, j in ((0, 0), (1, 1), (2, 2), (0, 1), (0, 2), (1, 2)):
        metric = (
            adjugate[i][0] * adjugate[j][0]
            + adjugate[i][1] * adjugate[j][1]
            + adjugate[i][2] * adjugate[j][2]
        )
        conduct.append(cross * metric + scaled[i] * pulled[j])
    return conduct


def stretch_of(entries, fiber):
    parts = [
        entries[3 * i] * fiber[0] + entries[3 * i + 1] * fiber[1] + entries[3 * i + 2] * fiber[2]
        for i in range(3)
    ]
    return jnp.sqrt(parts[0] * parts[0] + parts[1] * parts[1] + parts[2] * parts[2])


def gather_refined(held, q, chosen, page, weight_z, sizes, down):
    bx, by, nz, ex, ey, ez, parts, count = sizes
    blocks = count // LANES
    pages = down * blocks
    width = (ey + 2) * ez
    table = [held[q, h, 0 : 8 * blocks] for h in range(down)]
    table += [held[q, h, 8 * blocks : 9 * blocks] for h in range(down)]
    found = dot_two(jnp.concatenate(table, axis=0), chosen)
    total = jnp.zeros((8, width), jnp.float32)
    for h in range(pages):
        total = jnp.where(page == h, found[8 * h : 8 * h + 8], total)
    kept = lax.broadcasted_iota(jnp.int32, (pages, width), 0) == page
    last = jnp.sum(jnp.where(kept, found[8 * pages : 9 * pages], 0.0), axis=0, keepdims=True)
    row = lax.broadcasted_iota(jnp.int32, (8, width), 0)
    here = row == lax.broadcasted_iota(jnp.int32, (8, width), 1) // ez
    spread = [jnp.where(here, total[k : k + 1], 0.0) for k in range(8)]
    spread.append(jnp.where(here, last, 0.0))
    return dot_two(jnp.concatenate(spread, axis=0), weight_z)


def hat(distance):
    return jnp.maximum(1.0 - jnp.abs(distance), 0.0)


def exchange(
    across,
    down,
    sizes,
    potential,
    recovery,
    angles,
    deform,
    slots,
    volts,
    base,
    new_recovery,
    held,
    chosen,
    pages,
    fibers,
    rim_fibers,
    spread_xy,
    spread_z,
    own_refined,
    cells,
    rest_in,
    near_slots,
    send_sem,
    deform_sem,
    near_sem,
    local_sem,
):
    bx, by, nz, ex, ey, ez, parts, count = sizes
    blocks = count // LANES
    gx, gy = lax.axis_index("gx"), lax.axis_index("gy")
    first_x, last_x = gx == 0, gx == across - 1
    first_y, last_y = gy == 0, gy == down - 1

    def exists(dx, dy):
        checks = []
        if dx:
            checks.append(jnp.logical_not(first_x if dx < 0 else last_x))
        if dy:
            checks.append(jnp.logical_not(first_y if dy < 0 else last_y))
        return checks[0] if len(checks) == 1 else jnp.logical_and(*checks)

    barrier = pltpu.get_barrier_semaphore()

    def row_targets(dx):
        for step in range(0 if dx else 1, down):
            yield step, lax.rem(gy + step, down)

    def greet(dx):
        for _, target in row_targets(dx):
            pl.semaphore_signal(barrier, inc=1, device_id=(gx + dx, target), device_id_type=MESH)

    pl.when(exists(-1, 0))(lambda: greet(-1))
    pl.when(exists(1, 0))(lambda: greet(1))
    greet(0)

    packed = held.at[1, gy]
    local = []

    def fetch(source, target):
        copy = pltpu.make_async_copy(source, target, local_sem.at[len(local)])
        copy.start()
        local.append(copy)

    for b in range(blocks):
        columns = pl.ds(b * LANES, LANES)
        fetch(deform.at[pl.ds(0, 8), columns], packed.at[pl.ds(8 * b, 8)])
        fetch(deform.at[pl.ds(8, 1), columns], packed.at[pl.ds(8 * blocks + b, 1)])
    fetch(slots, near_slots.at[1, 1])
    inside = pl.ds(TOP, by)
    fetch(potential, cells.at[0, pl.ds(1, bx), inside])
    fetch(angles, cells.at[pl.ds(1, 2), pl.ds(1, bx), inside])
    fetch(recovery, rest_in)
    width = (ey + 2) * ez
    main = (bx + 2) * by
    row = lax.broadcasted_iota(jnp.int32, spread_xy.shape, 0)
    lane = lax.broadcasted_iota(jnp.int32, spread_xy.shape, 1)
    inner = row < main
    x_cell = jnp.where(inner, row // by - 1, lax.rem(row - main, bx))
    y_cell = jnp.where(inner, lax.rem(row, by), jnp.where(row < main + bx, -1, by))
    x_spot = (x_cell.astype(jnp.float32) + 0.5) * (1.0 / RATIO) + 0.5
    y_spot = (y_cell.astype(jnp.float32) + 0.5) * (1.0 / RATIO) + 0.5
    x_weight = hat(x_spot - (lax.rem(lane, 24) // 8).astype(jnp.float32))
    y_weight = hat(y_spot - lax.rem(lane, 8).astype(jnp.float32))
    spread_xy[...] = (x_weight * y_weight).astype(jnp.bfloat16)
    row = lax.broadcasted_iota(jnp.int32, (width, nz), 0)
    lane = lax.broadcasted_iota(jnp.int32, (width, nz), 1)
    spot = jnp.clip((lane.astype(jnp.float32) + 0.5) * (1.0 / RATIO) - 0.5, 0.0, ez - 1.0)
    spread_z[...] = hat(spot - lax.rem(row, ez).astype(jnp.float32)).astype(jnp.bfloat16)

    for copy in local:
        copy.wait()

    rows_here = 1 + jnp.where(first_x, 0, 1) + jnp.where(last_x, 0, 1)
    pl.semaphore_wait(barrier, rows_here * down - 1)

    def deform_copy(dx, step, target):
        index = (1 - dx) * down + step
        rows = pl.ds(0, 9 * blocks)
        return pltpu.make_async_remote_copy(
            src_ref=held.at[1, gy, rows],
            dst_ref=held.at[1 - dx, gy, rows],
            send_sem=send_sem.at[index],
            recv_sem=deform_sem.at[index],
            device_id=(gx + dx, target),
            device_id_type=MESH,
        )

    def near_copies(dx, dy):
        place = (1 - dx) * 3 + (1 - dy)
        base = 3 * down + 2 * place
        x_source = pl.ds(1, bx) if dx == 0 else pl.ds(1 if dx < 0 else bx, 1)
        x_target = pl.ds(1, bx) if dx == 0 else pl.ds(bx + 1 if dx < 0 else 0, 1)
        y_source = inside if dy == 0 else pl.ds(TOP if dy < 0 else TOP + by - 1, 1)
        y_target = inside if dy == 0 else pl.ds(TOP + by if dy < 0 else TOP - 1, 1)
        fields = pl.ds(0, 1 if dx and dy else 3)
        pairs = [
            (near_slots.at[1, 1], near_slots.at[1 - dx, 1 - dy]),
            (cells.at[fields, x_source, y_source], cells.at[fields, x_target, y_target]),
        ]
        return [
            pltpu.make_async_remote_copy(
                src_ref=source,
                dst_ref=target,
                send_sem=send_sem.at[base + number],
                recv_sem=near_sem.at[2 * place + number],
                device_id=(gx + dx, gy + dy),
                device_id_type=MESH,
            )
            for number, (source, target) in enumerate(pairs)
        ]

    def over_row(dx, act):
        for step, target in row_targets(dx):
            act(deform_copy(dx, step, target))

    def over_near(dx, dy, act):
        for copy in near_copies(dx, dy):
            act(copy)

    def far_rows(act, way=1):
        for dx in (-1, 1):
            pl.when(exists(way * dx, 0))(lambda dx=dx: over_row(dx, act))

    def all_near(act, way=1):
        for dx, dy in SIDES:
            pl.when(exists(way * dx, way * dy))(lambda dx=dx, dy=dy: over_near(dx, dy, act))

    all_near(lambda copy: copy.start())
    far_rows(lambda copy: copy.start())
    over_row(0, lambda copy: copy.start())

    def slice_fiber(s):
        angle = [cells[number, s, TOP : TOP + by] for number in (1, 2)]
        for number, part in enumerate(fiber_of(*angle)):
            fibers[number, s] = part

    for s in range(1, bx + 1):
        slice_fiber(s)
        voltage = cells[0, s, TOP : TOP + by]
        resting = rest_in[s - 1]
        current = 8.0 * voltage * (voltage - 0.15) * (voltage - 1.0) + voltage * resting
        base[s - 1] = voltage - 0.1 * current
        new_recovery[s - 1] = resting + 0.05 * (-resting - 8.0 * voltage * (voltage - 1.15))

    all_near(lambda copy: copy.wait_recv(), -1)

    volts[...] = cells[0]

    @pl.when(first_y)
    def _():
        volts[:, TOP - 1 : TOP] = volts[:, TOP : TOP + 1]

    @pl.when(last_y)
    def _():
        volts[:, TOP + by : TOP + by + 1] = volts[:, TOP + by - 1 : TOP + by]

    @pl.when(first_x)
    def _():
        volts[0] = volts[1]

    @pl.when(last_x)
    def _():
        volts[bx + 1] = volts[bx]

    slice_fiber(0)
    slice_fiber(bx + 1)

    def rim_of(number):
        rows = [
            cells[number, s + 1, row : row + 1] for row in (TOP - 1, TOP + by) for s in range(bx)
        ]
        return jnp.concatenate(rows, axis=0)

    for number, part in enumerate(fiber_of(rim_of(1), rim_of(2))):
        rim_fibers[number] = part

    digits = lax.broadcasted_iota(jnp.int32, (LANES, width), 0)
    for q in range(3):
        low = jnp.where(first_y, near_slots[q, 1, 0, 0:1], near_slots[q, 0, 0, ey - 1 : ey])
        high = jnp.where(last_y, near_slots[q, 1, 0, ey - 1 : ey], near_slots[q, 2, 0, 0:1])
        pieces = [low] + [near_slots[q, 1, 0, c : c + 1] for c in range(ey)] + [high]
        index = jnp.concatenate(pieces, axis=1) - (gx + q - 1) * (down * count)
        hit = digits == (index & (LANES - 1))
        chosen[q] = hit.astype(jnp.float32).astype(jnp.bfloat16)
        pages[q] = index >> (LANES.bit_length() - 1)

    over_row(0, lambda copy: copy.wait_recv())
    far_rows(lambda copy: copy.wait_recv(), -1)
    far_rows(lambda copy: copy.wait_send())
    over_row(0, lambda copy: copy.wait_send())
    all_near(lambda copy: copy.wait_send())


def compute(
    across,
    down,
    sizes,
    volts,
    base,
    new_recovery,
    held,
    chosen,
    pages,
    fibers,
    rim_fibers,
    spread_xy,
    spread_z,
    own_refined,
    next_potential,
    next_recovery,
    conducts,
    out_potential,
    out_sem,
):
    bx, by, nz, ex, ey, ez, parts, count = sizes
    blocks = count // LANES
    gx, gy = lax.axis_index("gx"), lax.axis_index("gy")
    first_x, last_x = gx == 0, gx == across - 1
    first_y, last_y = gy == 0, gy == down - 1
    leaving = [pltpu.make_async_copy(new_recovery, next_recovery, out_sem.at[bx])]
    leaving[0].start()

    weight_z = spread_z[...]
    own = gather_refined(held, 1, chosen[1], pages[1], weight_z, sizes, down)
    low, high = (
        gather_refined(held, q, chosen[q], pages[q], weight_z, sizes, down) for q in (0, 2)
    )
    low = jnp.where(first_x, own, low)
    high = jnp.where(last_x, own, high)
    weight_xy = spread_xy[...]
    refined = []
    for k in range(parts):
        rows = slice(8 * k, 8 * k + 8)
        stack = jnp.concatenate([low[rows], own[rows], high[rows]], axis=0)
        front = stack.astype(jnp.bfloat16).astype(jnp.float32)
        stack = jnp.concatenate([front, stack - front], axis=0).astype(jnp.bfloat16)
        refined.append(jnp.dot(weight_xy, stack, preferred_element_type=jnp.float32))

    for s in range(bx + 2):
        for half in range(by // 8):
            rows = slice(8 * half, 8 * half + 8)
            start = s * by + 8 * half
            entries = [refined[k][start : start + 8] for k in range(parts)]
            fiber = [fibers[number, s, rows] for number in range(3)]
            for number, value in enumerate(tensor_of(entries, fiber)):
                conducts[number, s, TOP + 8 * half : TOP + 8 * half + 8] = value
            if 1 <= s <= bx:
                out_potential[s - 1, rows] = stretch_of(entries, fiber)
    start = (bx + 2) * by
    entries = [refined[k][start : start + 2 * bx] for k in range(parts)]
    rim_fiber = [rim_fibers[number] for number in range(3)]
    for number, value in enumerate(tensor_of(entries, rim_fiber)):
        for s in range(bx):
            conducts[number, s + 1, TOP - 1 : TOP] = value[s : s + 1]
            conducts[number, s + 1, TOP + by : TOP + by + 1] = value[bx + s : bx + s + 1]

    z_lane = lax.broadcasted_iota(jnp.int32, (by, nz), 1)
    y_row = lax.broadcasted_iota(jnp.int32, (by, nz), 0)

    def next_z(values):
        return jnp.where(z_lane == nz - 1, values, pltpu.roll(values, nz - 1, 1))

    def last_z(values):
        return jnp.where(z_lane == 0, values, pltpu.roll(values, 1, 1))

    def grad_z(values):
        return next_z(values) - last_z(values)

    def at(s, shift):
        return volts[s, TOP + shift : TOP + shift + by]

    def tensor(number, s, shift=0):
        return conducts[number, s, TOP + shift : TOP + shift + by]

    XX, YY, ZZ, XY, XZ, YZ = range(6)
    middle = [at(s, 0) for s in range(bx + 2)]
    grads_y = [at(s, 1) - at(s, -1) for s in range(bx + 2)]
    grads_z = [grad_z(middle[s]) for s in range(bx + 2)]

    def face_x(f):
        def mean(number):
            return tensor(number, f) + tensor(number, f + 1)

        return (
            0.5 * mean(XX) * (middle[f + 1] - middle[f])
            + 0.125 * mean(XY) * (grads_y[f] + grads_y[f + 1])
            + 0.125 * mean(XZ) * (grads_z[f] + grads_z[f + 1])
        )

    faces = [face_x(f) for f in range(bx + 1)]
    faces[0] = jnp.where(first_x, 0.0, faces[0])
    faces[bx] = jnp.where(last_x, 0.0, faces[bx])

    for i in range(bx):
        s = i + 1
        grad_x = middle[s + 1] - middle[s - 1]

        def face_y(shift):
            def mean(number):
                return tensor(number, s) + tensor(number, s, shift)

            step = (at(s, shift) - middle[s]) * (1.0 if shift > 0 else -1.0)
            other_x = at(s + 1, shift) - at(s - 1, shift)
            return (
                0.125 * mean(XY) * (grad_x + other_x)
                + 0.5 * mean(YY) * step
                + 0.125 * mean(YZ) * (grads_z[s] + grad_z(at(s, shift)))
            )

        upper = jnp.where(jnp.logical_and(y_row == by - 1, last_y), 0.0, face_y(1))
        lower = jnp.where(jnp.logical_and(y_row == 0, first_y), 0.0, face_y(-1))

        def pair(values):
            return values + next_z(values)

        face_z = (
            0.125 * pair(tensor(XZ, s)) * pair(grad_x)
            + 0.125 * pair(tensor(YZ, s)) * pair(grads_y[s])
            + 0.5 * pair(tensor(ZZ, s)) * (next_z(middle[s]) - middle[s])
        )
        face_z = jnp.where(z_lane == nz - 1, 0.0, face_z)
        divergent = (
            (faces[i + 1] - faces[i]) + (upper - lower) + (face_z - pltpu.roll(face_z, 1, 1))
        )
        extra = jnp.maximum(out_potential[i] - 1.0, 0.0) * (middle[s] - 0.6)
        out_potential[i] = base[i] + 0.1 * divergent - extra
        copy = pltpu.make_async_copy(out_potential.at[i], next_potential.at[i], out_sem.at[i])
        copy.start()
        leaving.append(copy)
    for copy in leaving:
        copy.wait()


def solution(mesh):
    across, down = mesh.shape["gx"], mesh.shape["gy"]

    def local(potential, recovery, angles, deform, slots):
        bx, by, nz = potential.shape
        ex, ey, ez = slots.shape
        parts, count = deform.shape
        assert ex == 1 and bx == RATIO and by % 8 == 0 and count % LANES == 0 and parts == 9 and 4 < ey + 2 <= 8
        sizes = (bx, by, nz, ex, ey, ez, parts, count)
        blocks = count // LANES
        width = (ey + 2) * ez
        f32 = jnp.float32
        shape = jax.ShapeDtypeStruct(potential.shape, f32)
        anywhere = pl.BlockSpec(memory_space=pl.ANY)
        in_vmem = pl.BlockSpec(memory_space=pltpu.VMEM)
        passed = (
            pltpu.VMEM((bx + 2, by + 16, nz), f32),
            pltpu.VMEM(recovery.shape, f32),
            pltpu.VMEM(recovery.shape, f32),
            pltpu.VMEM((3, down, 8 * blocks + 8, LANES), f32),
            pltpu.VMEM((3, LANES, width), jnp.bfloat16),
            pltpu.VMEM((3, 1, width), jnp.int32),
            pltpu.VMEM((3, bx + 2, by, nz), f32),
            pltpu.VMEM((3, 2 * bx, nz), f32),
            pltpu.VMEM(((bx + 2) * by + 2 * bx + 8, 48), jnp.bfloat16),
            pltpu.VMEM((width, nz), jnp.bfloat16),
            pltpu.VMEM((8 * parts, nz), f32),
        )
        arrived = pl.pallas_call(
            functools.partial(exchange, across, down, sizes),
            out_shape=passed,
            in_specs=[pl.BlockSpec(memory_space=pltpu.MemorySpace.HBM)] * 5,
            out_specs=(in_vmem,) * len(passed),
            scratch_shapes=[
                pltpu.VMEM((3, bx + 2, by + 16, nz), f32),
                pltpu.VMEM(recovery.shape, f32),
                pltpu.VMEM((3, 3, ex, ey, ez), jnp.int32),
                pltpu.SemaphoreType.DMA((3 * down + 18,)),
                pltpu.SemaphoreType.DMA((3 * down,)),
                pltpu.SemaphoreType.DMA((18,)),
                pltpu.SemaphoreType.DMA((2 * blocks + 4,)),
            ],
            compiler_params=pltpu.CompilerParams(
                collective_id=0, has_side_effects=True, vmem_limit_bytes=VMEM_LIMIT
            ),
        )(*(pltpu.with_memory_space_constraint(x, pltpu.MemorySpace.HBM) for x in (potential, recovery, angles, deform, slots)))
        return pl.pallas_call(
            functools.partial(compute, across, down, sizes),
            out_shape=(shape, shape),
            in_specs=[in_vmem] * len(passed),
            out_specs=(anywhere,) * 2,
            scratch_shapes=[
                pltpu.VMEM((6, bx + 2, by + 16, nz), f32),
                pltpu.VMEM((bx, by, nz), f32),
                pltpu.SemaphoreType.DMA((bx + 1,)),
            ],
            compiler_params=pltpu.CompilerParams(vmem_limit_bytes=VMEM_LIMIT),
        )(*arrived)

    return jax.shard_map(
        local,
        mesh=mesh,
        in_specs=(
            P("gx", "gy", None),
            P("gx", "gy", None),
            P(None, "gx", "gy", None),
            P(None, ("gx", "gy")),
            P("gx", "gy", None),
        ),
        out_specs=(P("gx", "gy", None), P("gx", "gy", None)),
        check_vma=False,
    )
```
